32 devices in a mesh: gx: 8 (over z, x), gy: 4 (over y, core).
Axes of the slice: x: 2, y: 2, z: 4, core: 2. Of those that a mesh axis runs over, the one named last changes fastest.
Arguments:
- velocity: float32 [3, 64, 256, 256], P(None, 'gx', 'gy'), may hold values from -10 to 10
Outputs:
- coefficient: float32 [256], P('gy')
- viscosity: float32 [64, 256, 256], P('gx', 'gy')
The draws below stay inside these ranges and needn't reach their ends.
All inputs are finite; a program needn't handle non-finite values.
Results may differ from the reference program's by a relative error of at most 0.00002.
Values sent between devices are 32-bit elements; how exact they have to be, the bound alone decides.
A program may use at most 64 MiB of HBM per device.

```python
import jax
import jax.numpy as jnp
from jax import lax

NZ = 256
NX = 64
NY = 256


def draw_velocity(key, part):
    noise_key = jax.random.fold_in(key, 0)
    stream_pos = jnp.arange(NX, dtype=jnp.float32) / NX
    wall_pos = (jnp.arange(NY, dtype=jnp.float32) + 0.5) / NY
    amplitude = (0.5 + stream_pos)[:, None, None] * (0.5 + wall_pos)[None, :, None]
    fluctuation = jax.random.normal(noise_key, (3, NX, NY, NZ), jnp.float32)
    mean_flow = 6.0 * wall_pos * (1.0 - wall_pos)
    mean_field = jnp.stack([mean_flow, 0.0 * mean_flow, 0.0 * mean_flow])
    velocity_field = amplitude[None] * fluctuation + mean_field[:, None, :, None]
    return jnp.clip(velocity_field, -10.0, 10.0)


def setup_inputs(seed: int = 0) -> dict:
    arg_keys = jax.random.split(jax.random.key(seed), 2)
    velocity = draw_velocity(jax.random.fold_in(arg_keys[1], 71), 0)
    return {"velocity": velocity}


step_stream = 2.0
step_wall = 0.5
step_span = 1.0
clip_high = 0.1
weights = (1.0, 1.0, 1.0, 2.0, 2.0, 2.0)
index_pairs = ((0, 0), (1, 1), (2, 2), (0, 1), (0, 2), (1, 2))

def strain_inner(padded):
    grad_stream = (padded[:, 2:, 1:-1] - padded[:, :-2, 1:-1]) * (0.5 / step_stream)
    grad_wall = (padded[:, 1:-1, 2:] - padded[:, 1:-1, :-2]) * (0.5 / step_wall)
    centre = padded[:, 1:-1, 1:-1]
    grad_span = (jnp.roll(centre, -1, 3) - jnp.roll(centre, 1, 3)) * (0.5 / step_span)
    gradients = (grad_stream, grad_wall, grad_span)
    return jnp.stack([0.5 * (gradients[second][first] + gradients[first][second]) for first, second in index_pairs])

def weight_column():
    return jnp.asarray(weights, jnp.float32).reshape(6, 1, 1, 1)

def magnitude(strain):
    return jnp.sqrt(2.0 * lax.optimization_barrier(jnp.sum(weight_column() * strain * strain, axis=0)))

def test_filter(field):
    smoothed = 0.25 * field[:, :-2] + 0.5 * field[:, 1:-1] + 0.25 * field[:, 2:]
    return 0.25 * jnp.roll(smoothed, 1, 3) + 0.5 * smoothed + 0.25 * jnp.roll(smoothed, -1, 3)

def plane_sums(velocity_pad, stress_pad, filtered_pad):
    strain_hat = strain_inner(filtered_pad)
    magnitude_hat = magnitude(strain_hat)
    row_values = velocity_pad[:, :, 1:-1]
    products = jnp.stack([row_values[first] * row_values[second] for first, second in index_pairs])
    product_hat = test_filter(products)
    centre = filtered_pad[:, 1:-1, 1:-1]
    leonard = product_hat - jnp.stack([centre[first] * centre[second] for first, second in index_pairs])
    trace_third = (leonard[0] + leonard[1] + leonard[2]) / 3.0
    leonard = jnp.concatenate([leonard[:3] - trace_third[None], leonard[3:]])
    model_tensor = 2.0 * (test_filter(stress_pad) - 4.0 * magnitude_hat[None] * strain_hat)
    numerator = lax.optimization_barrier(jnp.sum(weight_column() * leonard * model_tensor, axis=(0, 1, 3)))
    denominator = lax.optimization_barrier(jnp.sum(weight_column() * model_tensor * model_tensor, axis=(0, 1, 3)))
    return (numerator, denominator)

def wrap_stream(field):
    return jnp.concatenate([field[:, -1:], field, field[:, :1]], axis=1)

def pad_walls(field):
    return jnp.pad(field, ((0, 0), (0, 0), (1, 1), (0, 0)))

def reference(velocity):
    velocity_pad = pad_walls(wrap_stream(velocity))
    strain = strain_inner(velocity_pad)
    strength = magnitude(strain)
    stress = strength[None] * strain
    filtered = test_filter(velocity_pad[:, :, 1:-1])
    filtered_pad = pad_walls(wrap_stream(filtered))
    stress_pad = wrap_stream(stress)
    numerator, denominator = plane_sums(velocity_pad, stress_pad, filtered_pad)
    raw_profile = jnp.clip(numerator / denominator, 0.0, clip_high)
    rim_values = jnp.concatenate([raw_profile[:1], raw_profile, raw_profile[-1:]])
    smooth = 0.25 * rim_values[:-2] + 0.5 * raw_profile + 0.25 * rim_values[2:]
    return (smooth, smooth[None, :, None] * strength)
```

```python
import functools

import jax
import jax.numpy as jnp
from jax import lax
from jax.experimental import pallas as pl
from jax.experimental.pallas import tpu as pltpu
from jax.sharding import PartitionSpec as P

clip_high = 0.1
pairs = ((0, 0), (1, 1), (2, 2), (0, 1), (0, 2), (1, 2))
MESH = pl.DeviceIdType.MESH
EARLY = 3


def tile(index):
    return pl.ds(pl.multiple_of(index * 8, 8), 8)


def roll_next(value):
    return pltpu.roll(value, value.shape[1] - 1, 1)


def roll_prev(value):
    return pltpu.roll(value, 1, 1)


def filter_span(value):
    pair = value + roll_next(value)
    return pair + roll_prev(pair)


def slope_span(value):
    step = roll_next(value) - value
    return step + roll_prev(step)


def slope_wall(ref, comp, row, t, here):
    rows = lax.broadcasted_iota(jnp.int32, here.shape, 0)
    below = ref[comp, row, tile(t - 1), :]
    above = ref[comp, row, tile(t + 1), :]
    up = pltpu.roll(jnp.where(rows == 0, above, here), 7, 0)
    down = pltpu.roll(jnp.where(rows == 7, below, here), 1, 0)
    return up - down


def strain4(ref, row, t):
    here = [ref[c, row, tile(t), :] for c in range(3)]
    dx = [ref[c, row + 1, tile(t), :] - ref[c, row - 1, tile(t), :] for c in range(3)]
    dy = [slope_wall(ref, c, row, t, here[c]) for c in range(3)]
    dz = [slope_span(here[c]) for c in range(3)]
    s = (
        dx[0],
        4.0 * dy[1],
        2.0 * dz[2],
        2.0 * dy[0] + 0.5 * dx[1],
        dz[0] + 0.5 * dx[2],
        dz[1] + 2.0 * dy[2],
    )
    diag = s[0] * s[0] + s[1] * s[1] + s[2] * s[2]
    off = s[3] * s[3] + s[4] * s[4] + s[5] * s[5]
    return here, s, diag + 2.0 * off


def kernel(n, m, nx, ny, u_hbm, strength_hbm, coef_ref, u, w, v, q, g, strength, accn, accd,
           edge_out, edge_in, mine, gather, own_sem, out_sem, xs_send, xs_recv, ys_send, ys_recv,
           c_send, c_recv, g_send, g_recv):
    nt = ny // 8
    gx = lax.axis_index("gx")
    gy = lax.axis_index("gy")
    left, right = lax.rem(gx + n - 1, n), lax.rem(gx + 1, n)
    not_low, not_high = gy > 0, gy < m - 1
    lanes = mine.shape[-1]

    own = pltpu.make_async_copy(u_hbm, u.at[:, 2:2 + nx, 8:8 + ny, :], own_sem)
    own.start()

    barrier = pltpu.get_barrier_semaphore()

    def greet(i, carry):
        @pl.when(i != gx)
        def _():
            pl.semaphore_signal(barrier, inc=1, device_id=(i, gy), device_id_type=MESH)

        @pl.when(not_low)
        def _():
            pl.semaphore_signal(barrier, inc=1, device_id=(i, gy - 1), device_id_type=MESH)

        @pl.when(not_high)
        def _():
            pl.semaphore_signal(barrier, inc=1, device_id=(i, gy + 1), device_id_type=MESH)

        return carry

    lax.fori_loop(0, n, greet, 0)
    peers = jnp.where(not_low, n, 0) + jnp.where(not_high, n, 0) + (n - 1)
    pl.semaphore_wait(barrier, peers)

    def x_copy(side, t):
        src = 0 if side == 0 else nx - 2
        dst = nx + 2 if side == 0 else 0
        return pltpu.make_async_remote_copy(
            src_ref=u_hbm.at[:, src:src + 2, tile(t - 1), :],
            dst_ref=u.at[:, dst:dst + 2, tile(t), :],
            send_sem=xs_send.at[side, t - 1],
            recv_sem=xs_recv.at[side, t - 1],
            device_id=(left if side == 0 else right, gy),
            device_id_type=MESH,
        )

    def y_copy(side):
        src = 0 if side == 0 else ny - 8
        dst = ny + 8 if side == 0 else 0
        return pltpu.make_async_remote_copy(
            src_ref=u_hbm.at[:, :, src:src + 8, :],
            dst_ref=u.at[:, 2:2 + nx, dst:dst + 8, :],
            send_sem=ys_send.at[side],
            recv_sem=ys_recv.at[side],
            device_id=(gx, gy - 1 if side == 0 else gy + 1),
            device_id_type=MESH,
        )

    def c_copy(side):
        return pltpu.make_async_remote_copy(
            src_ref=edge_out.at[side],
            dst_ref=edge_in.at[side],
            send_sem=c_send.at[side],
            recv_sem=c_recv.at[side],
            device_id=(left if side == 0 else right, gy),
            device_id_type=MESH,
        )

    @pl.when(not_low)
    def _():
        y_copy(0).start()

    @pl.when(not_high)
    def _():
        y_copy(1).start()

    def start_x(t, carry):
        x_copy(0, t).start()
        x_copy(1, t).start()
        return carry

    lax.fori_loop(1, 1 + EARLY, start_x, 0)

    accn[...] = jnp.zeros_like(accn)
    accd[...] = jnp.zeros_like(accd)

    @pl.when(jnp.logical_not(not_low))
    def _():
        u[:, 2:2 + nx, 0:8, :] = jnp.zeros((3, nx, 8, u.shape[3]), jnp.float32)

    @pl.when(jnp.logical_not(not_high))
    def _():
        u[:, 2:2 + nx, ny + 8:ny + 16, :] = jnp.zeros((3, nx, 8, u.shape[3]), jnp.float32)

    @pl.when(not_high)
    def _():
        y_copy(0).wait_recv()

    @pl.when(not_low)
    def _():
        y_copy(1).wait_recv()

    for side in range(2):
        src = 2 if side == 0 else nx
        for c in range(3):
            for r in range(2):
                k = 2 * c + r
                edge_out[side, k:k + 1, :] = u[c, src + r, 7:8, :]
                edge_out[side, 8 + k:9 + k, :] = u[c, src + r, ny + 8:ny + 9, :]
    own.wait()
    for side in range(2):
        c_copy(side).start()
    lax.fori_loop(1 + EARLY, nt + 1, start_x, 0)

    def span_rows(t, rows):
        for c in range(3):
            for row in rows:
                w[c, row, tile(t), :] = filter_span(u[c, row, tile(t), :])

    def filtered_rows(t, rows):
        for c in range(3):
            for row in rows:
                a, b, d = (w[c, row + k, tile(t), :] for k in (-1, 0, 1))
                v[c, row, tile(t), :] = 0.25 * ((a + b) + (b + d))

    def stress_row(t, row, keep):
        here, s, total = strain4(u, row, t)
        size = jnp.sqrt(0.125 * total)
        if keep:
            strength[row - 2, tile(t - 1), :] = size
        for k, (a, b) in enumerate(pairs):
            q[k, row, tile(t - 1), :] = filter_span(here[a] * here[b])
            g[k, row, tile(t - 1), :] = filter_span(size * s[k])

    def sums_row(t, row):
        centre, s, total = strain4(v, row, t)
        scale = jnp.sqrt(2.0 * total)

        def stream(ref, k):
            a, b, d = (ref[k, row + j, tile(t - 1), :] for j in (-1, 0, 1))
            return (a + b) + (b + d)

        leonard = [stream(q, k) - centre[a] * centre[b] for k, (a, b) in enumerate(pairs)]
        third = (leonard[0] + leonard[1] + leonard[2]) * (1.0 / 3.0)
        leonard = [x - third for x in leonard[:3]] + leonard[3:]
        model = [stream(g, k) - scale * s[k] for k in range(6)]
        lm = [x * y for x, y in zip(leonard, model)]
        mm = [x * x for x in model]
        num = (lm[0] + lm[1] + lm[2]) + 2.0 * (lm[3] + lm[4] + lm[5])
        den = (mm[0] + mm[1] + mm[2]) + 2.0 * (mm[3] + mm[4] + mm[5])
        return num, den

    def fold(value):
        parts = [value[:, k:k + 128] for k in range(0, value.shape[1], 128)]
        return functools.reduce(lambda x, y: x + y, parts)

    def sums(t, rows):
        both = [sums_row(t, row) for row in rows]
        num = functools.reduce(lambda x, y: x + y, [b[0] for b in both])
        den = functools.reduce(lambda x, y: x + y, [b[1] for b in both])
        accn[tile(t - 1), :] += fold(num)
        accd[tile(t - 1), :] += fold(den)

    def inner_filter(t, carry):
        span_rows(t, range(2, nx + 2))
        filtered_rows(t, range(3, nx + 1))
        return carry

    lax.fori_loop(0, nt + 2, inner_filter, 0)

    half = (nx - 2) // 2

    def inner_stress(i, carry):
        t = i // half + 1
        row = 3 + 2 * lax.rem(i, half)
        stress_row(t, row, True)
        stress_row(t, row + 1, True)
        return carry

    lax.fori_loop(0, nt * half, inner_stress, 0)

    less = (nx - 4) // 2

    def inner_sums(i, carry):
        t = i // less + 1
        row = 4 + 2 * lax.rem(i, less)
        sums(t, (row, row + 1))
        return carry

    lax.fori_loop(0, nt * less, inner_sums, 0)
    inner_out = pltpu.make_async_copy(
        strength.at[1:nx - 1], strength_hbm.at[1:nx - 1], out_sem.at[0]
    )
    inner_out.start()

    def rim_first(t):
        span_rows(t, (0, 1, nx + 2, nx + 3))
        filtered_rows(t, (1, 2, nx + 1, nx + 2))

    def rim_second(t):
        for row in (1, 2, nx + 1, nx + 2):
            stress_row(t, row, row in (2, nx + 1))
        sums(t, (2, 3, nx, nx + 1))

    def arrive(t, carry):
        x_copy(0, t).wait_recv()
        x_copy(1, t).wait_recv()
        rim_first(t)
        return carry

    lax.fori_loop(1, 1 + EARLY, arrive, 0)
    for side in range(2):
        c_copy(side).wait_recv()
    for side in range(2):
        dst = nx + 2 if side == 0 else 0
        for c in range(3):
            for r in range(2):
                k = 2 * c + r
                u[c, dst + r, 7:8, :] = edge_in[side, k:k + 1, :]
                u[c, dst + r, ny + 8:ny + 9, :] = edge_in[side, 8 + k:9 + k, :]

    def rim_ends(i, carry):
        rim_first(i * (nt + 1))
        return carry

    lax.fori_loop(0, 2, rim_ends, 0)

    def finish(t, carry):
        @pl.when(jnp.logical_and(t > EARLY, t <= nt))
        def _():
            arrive(t, 0)

        rim_second(t - 1)
        return carry

    lax.fori_loop(2, nt + 2, finish, 0)
    rim_out = []
    for k, row in enumerate((0, nx - 1)):
        copy = pltpu.make_async_copy(
            strength.at[row], strength_hbm.at[row], out_sem.at[1 + k]
        )
        copy.start()
        rim_out.append(copy)

    mine[0:1, :] = jnp.sum(accn[...].T, axis=0, keepdims=True)
    mine[1:2, :] = jnp.sum(accd[...].T, axis=0, keepdims=True)

    def g_copy(kind, to_x, to_y, from_x):
        return pltpu.make_async_remote_copy(
            src_ref=mine,
            dst_ref=gather.at[kind, from_x],
            send_sem=g_send.at[kind, to_x],
            recv_sem=g_recv.at[kind, from_x],
            device_id=(to_x, to_y),
            device_id_type=MESH,
        )

    def send(i, carry):
        @pl.when(i != gx)
        def _():
            g_copy(0, i, gy, gx).start()

        @pl.when(not_low)
        def _():
            g_copy(2, i, gy - 1, gx).start()

        @pl.when(not_high)
        def _():
            g_copy(1, i, gy + 1, gx).start()

        return carry

    lax.fori_loop(0, n, send, 0)
    gather[0, gx] = mine[...]

    def take(i, carry):
        @pl.when(i != gx)
        def _():
            g_copy(0, i, gy, i).wait_recv()

        @pl.when(not_low)
        def _():
            g_copy(1, i, gy, i).wait_recv()

        @pl.when(not_high)
        def _():
            g_copy(2, i, gy, i).wait_recv()

        return carry

    lax.fori_loop(0, n, take, 0)

    def profile(kind):
        def add(i, total):
            return total + gather[kind, i]

        total = lax.fori_loop(0, n, add, jnp.zeros((2, lanes), jnp.float32))
        return jnp.clip(2.0 * (total[0:1] / total[1:2]), 0.0, clip_high)

    raw = profile(0)
    where = lax.broadcasted_iota(jnp.int32, (1, lanes), 1)
    first = where == 0
    last = where == ny - 1
    under = jnp.where(first, raw, pltpu.roll(raw, 1, 1))
    over = jnp.where(last, raw, pltpu.roll(raw, lanes - 1, 1))
    low_raw = pltpu.roll(profile(1), (lanes + 1 - ny) % lanes, 1)
    high_raw = pltpu.roll(profile(2), ny - 1, 1)
    under = jnp.where(jnp.logical_and(first, not_low), low_raw, under)
    over = jnp.where(jnp.logical_and(last, not_high), high_raw, over)
    coef_ref[...] = 0.25 * under + 0.5 * raw + 0.25 * over

    def left_x(t, carry):
        x_copy(0, t).wait_send()
        x_copy(1, t).wait_send()
        return carry

    lax.fori_loop(1, nt + 1, left_x, 0)
    for side in range(2):
        c_copy(side).wait_send()

    @pl.when(not_low)
    def _():
        y_copy(0).wait_send()

    @pl.when(not_high)
    def _():
        y_copy(1).wait_send()

    def left_g(i, carry):
        @pl.when(i != gx)
        def _():
            g_copy(0, i, gy, gx).wait_send()

        @pl.when(not_low)
        def _():
            g_copy(2, i, gy - 1, gx).wait_send()

        @pl.when(not_high)
        def _():
            g_copy(1, i, gy + 1, gx).wait_send()

        return carry

    lax.fori_loop(0, n, left_g, 0)
    inner_out.wait()
    for copy in rim_out:
        copy.wait()


def local(n, m, velocity):
    _, nx, ny, nz = velocity.shape
    lanes = -(-ny // 128) * 128
    nt = ny // 8
    f32 = jnp.float32
    strength, coef = pl.pallas_call(
        functools.partial(kernel, n, m, nx, ny),
        out_shape=(
            jax.ShapeDtypeStruct((nx, ny, nz), f32),
            jax.ShapeDtypeStruct((1, lanes), f32),
        ),
        in_specs=[pl.BlockSpec(memory_space=pl.ANY)],
        out_specs=(
            pl.BlockSpec(memory_space=pl.ANY),
            pl.BlockSpec(memory_space=pltpu.VMEM),
        ),
        scratch_shapes=[
            pltpu.VMEM((3, nx + 4, ny + 16, nz), f32),
            pltpu.VMEM((3, nx + 4, ny + 16, nz), f32),
            pltpu.VMEM((3, nx + 4, ny + 16, nz), f32),
            pltpu.VMEM((6, nx + 4, ny, nz), f32),
            pltpu.VMEM((6, nx + 4, ny, nz), f32),
            pltpu.VMEM((nx, ny, nz), f32),
            pltpu.VMEM((lanes, 128), f32),
            pltpu.VMEM((lanes, 128), f32),
            pltpu.VMEM((2, 16, nz), f32),
            pltpu.VMEM((2, 16, nz), f32),
            pltpu.VMEM((2, lanes), f32),
            pltpu.VMEM((3, n, 2, lanes), f32),
            pltpu.SemaphoreType.DMA,
            pltpu.SemaphoreType.DMA((3,)),
            pltpu.SemaphoreType.DMA((2, nt)),
            pltpu.SemaphoreType.DMA((2, nt)),
            pltpu.SemaphoreType.DMA((2,)),
            pltpu.SemaphoreType.DMA((2,)),
            pltpu.SemaphoreType.DMA((2,)),
            pltpu.SemaphoreType.DMA((2,)),
            pltpu.SemaphoreType.DMA((3, n)),
            pltpu.SemaphoreType.DMA((3, n)),
        ],
        compiler_params=pltpu.CompilerParams(
            collective_id=0, has_side_effects=True, vmem_limit_bytes=48 * 1024 * 1024
        ),
    )(velocity)
    smooth = coef[0, :ny]
    return (smooth, smooth[None, :, None] * strength)


def solution(mesh):
    n, m = mesh.shape["gx"], mesh.shape["gy"]
    return jax.shard_map(
        functools.partial(local, n, m),
        mesh=mesh,
        in_specs=(P(None, "gx", "gy", None),),
        out_specs=(P("gy"), P("gx", "gy", None)),
        check_vma=False,
    )
```

```python
import functools

import jax
import jax.numpy as jnp
from jax import lax
from jax.experimental import pallas as pl
from jax.experimental.pallas import tpu as pltpu
from jax.sharding import PartitionSpec as P

clip_high = 0.1
pairs = ((0, 0), (1, 1), (2, 2), (0, 1), (0, 2), (1, 2))
MESH = pl.DeviceIdType.MESH
EARLY = 3


def tile(index):
    return pl.ds(pl.multiple_of(index * 8, 8), 8)


def roll_next(value):
    return pltpu.roll(value, value.shape[1] - 1, 1)


def roll_prev(value):
    return pltpu.roll(value, 1, 1)


def filter_span(value):
    return (roll_next(value) + roll_prev(value)) + 2.0 * value


def slope_span(value):
    return roll_next(value) - roll_prev(value)


def slope_wall(ref, comp, row, t, here):
    rows = lax.broadcasted_iota(jnp.int32, here.shape, 0)
    below = ref[comp, row, tile(t - 1), :]
    above = ref[comp, row, tile(t + 1), :]
    up = pltpu.roll(jnp.where(rows == 0, above, here), 7, 0)
    down = pltpu.roll(jnp.where(rows == 7, below, here), 1, 0)
    return up - down


def strain4(ref, row, t, slope=None):
    here = [ref[c, row, tile(t), :] for c in range(3)]
    dx = [ref[c, row + 1, tile(t), :] - ref[c, row - 1, tile(t), :] for c in range(3)]
    dy = [slope_wall(ref, c, row, t, here[c]) for c in range(3)]
    if slope is None:
        dz = [slope_span(here[c]) for c in range(3)]
    else:
        dz = [slope[c, row, tile(t), :] for c in range(3)]
    s = (
        dx[0],
        4.0 * dy[1],
        2.0 * dz[2],
        2.0 * dy[0] + 0.5 * dx[1],
        dz[0] + 0.5 * dx[2],
        dz[1] + 2.0 * dy[2],
    )
    diag = s[0] * s[0] + s[1] * s[1] + s[2] * s[2]
    off = s[3] * s[3] + s[4] * s[4] + s[5] * s[5]
    return here, s, diag + 2.0 * off


def kernel(n, m, nx, ny, u_hbm, strength_hbm, coef_ref, u, w, v, d, g, strength, accn, accd,
           edge_out, edge_in, mine, gather, own_sem, out_sem, xs_send, xs_recv, ys_send, ys_recv,
           c_send, c_recv, g_send, g_recv, ring):
    nt = ny // 8
    gx = lax.axis_index("gx")
    gy = lax.axis_index("gy")
    left, right = lax.rem(gx + n - 1, n), lax.rem(gx + 1, n)
    not_low, not_high = gy > 0, gy < m - 1
    lanes = mine.shape[-1]

    own = pltpu.make_async_copy(u_hbm, u.at[:, 2:2 + nx, 8:8 + ny, :], own_sem)
    own.start()

    barrier = pltpu.get_barrier_semaphore()

    def to_ends(semaphore):
        @pl.when(not_low)
        def _():
            pl.semaphore_signal(semaphore, inc=1, device_id=(gx, gy - 1), device_id_type=MESH)

        @pl.when(not_high)
        def _():
            pl.semaphore_signal(semaphore, inc=1, device_id=(gx, gy + 1), device_id_type=MESH)

    def to_sides(semaphore):
        for side in (left, right):
            pl.semaphore_signal(semaphore, inc=1, device_id=(side, gy), device_id_type=MESH)

    to_sides(barrier)
    to_ends(barrier)
    ends = jnp.where(not_low, 1, 0) + jnp.where(not_high, 1, 0)
    pl.semaphore_wait(barrier, ends + 2)

    rounds = n // 2 - 1

    def open_round(k):
        if k < rounds:
            to_sides(ring.at[k])

    def close_round(k):
        if k < rounds:
            pl.semaphore_wait(ring.at[k], 2)

    def x_copy(side, t):
        src = 0 if side == 0 else nx - 2
        dst = nx + 2 if side == 0 else 0
        return pltpu.make_async_remote_copy(
            src_ref=u_hbm.at[:, src:src + 2, tile(t - 1), :],
            dst_ref=u.at[:, dst:dst + 2, tile(t), :],
            send_sem=xs_send.at[side, t - 1],
            recv_sem=xs_recv.at[side, t - 1],
            device_id=(left if side == 0 else right, gy),
            device_id_type=MESH,
        )

    def y_copy(side):
        src = 0 if side == 0 else ny - 8
        dst = ny + 8 if side == 0 else 0
        return pltpu.make_async_remote_copy(
            src_ref=u_hbm.at[:, :, src:src + 8, :],
            dst_ref=u.at[:, 2:2 + nx, dst:dst + 8, :],
            send_sem=ys_send.at[side],
            recv_sem=ys_recv.at[side],
            device_id=(gx, gy - 1 if side == 0 else gy + 1),
            device_id_type=MESH,
        )

    def c_copy(side):
        return pltpu.make_async_remote_copy(
            src_ref=edge_out.at[side],
            dst_ref=edge_in.at[side],
            send_sem=c_send.at[side],
            recv_sem=c_recv.at[side],
            device_id=(left if side == 0 else right, gy),
            device_id_type=MESH,
        )

    @pl.when(not_low)
    def _():
        y_copy(0).start()

    @pl.when(not_high)
    def _():
        y_copy(1).start()

    def start_x(t, carry):
        x_copy(0, t).start()
        x_copy(1, t).start()
        return carry

    lax.fori_loop(1, 1 + EARLY, start_x, 0)

    accn[...] = jnp.zeros_like(accn)
    accd[...] = jnp.zeros_like(accd)

    @pl.when(jnp.logical_not(not_low))
    def _():
        u[:, 2:2 + nx, 0:8, :] = jnp.zeros((3, nx, 8, u.shape[3]), jnp.float32)

    @pl.when(jnp.logical_not(not_high))
    def _():
        u[:, 2:2 + nx, ny + 8:ny + 16, :] = jnp.zeros((3, nx, 8, u.shape[3]), jnp.float32)

    @pl.when(not_high)
    def _():
        y_copy(0).wait_recv()

    @pl.when(not_low)
    def _():
        y_copy(1).wait_recv()

    for side in range(2):
        src = 2 if side == 0 else nx
        for c in range(3):
            for r in range(2):
                k = 2 * c + r
                edge_out[side, k:k + 1, :] = u[c, src + r, 7:8, :]
                edge_out[side, 8 + k:9 + k, :] = u[c, src + r, ny + 8:ny + 9, :]
    own.wait()
    for side in range(2):
        c_copy(side).start()
    lax.fori_loop(1 + EARLY, nt + 1, start_x, 0)

    def span_rows(t, rows, slopes=True):
        for c in range(3):
            for row in rows:
                here = u[c, row, tile(t), :]
                after, before = roll_next(here), roll_prev(here)
                w[c, row, tile(t), :] = (after + before) + 2.0 * here
                if slopes:
                    d[c, row, tile(t), :] = after - before

    def filtered_rows(t, rows):
        for c in range(3):
            for row in rows:
                a, b, e = (w[c, row + k, tile(t), :] for k in (-1, 0, 1))
                v[c, row, tile(t), :] = 0.25 * ((a + e) + 2.0 * b)

    def stress_row(t, row, keep):
        _, s, total = strain4(u, row, t, d)
        size = jnp.sqrt(0.125 * total)
        if keep:
            strength[row - 2, tile(t - 1), :] = size
        for k in range(6):
            g[k, row, tile(t - 1), :] = size * s[k]

    def sums_row(t, row):
        centre, s, total = strain4(v, row, t)
        scale = jnp.sqrt(2.0 * total)

        def product(a, b):
            one, two, three = (near[j][a] * near[j][b] for j in range(3))
            return filter_span((one + three) + 2.0 * two)

        def stress(k):
            one, two, three = (g[k, row + j, tile(t - 1), :] for j in (-1, 0, 1))
            return filter_span((one + three) + 2.0 * two)

        near = [[u[c, row + j, tile(t), :] for c in range(3)] for j in (-1, 0, 1)]
        leonard = [product(a, b) - centre[a] * centre[b] for a, b in pairs]
        third = (leonard[0] + leonard[1] + leonard[2]) * (1.0 / 3.0)
        leonard = [x - third for x in leonard[:3]] + leonard[3:]
        model = [stress(k) - scale * s[k] for k in range(6)]
        lm = [x * y for x, y in zip(leonard, model)]
        mm = [x * x for x in model]
        num = (lm[0] + lm[1] + lm[2]) + 2.0 * (lm[3] + lm[4] + lm[5])
        den = (mm[0] + mm[1] + mm[2]) + 2.0 * (mm[3] + mm[4] + mm[5])
        return num, den

    def fold(value):
        parts = [value[:, k:k + 128] for k in range(0, value.shape[1], 128)]
        return functools.reduce(lambda x, y: x + y, parts)

    def sums(t, rows):
        both = [sums_row(t, row) for row in rows]
        num = functools.reduce(lambda x, y: x + y, [b[0] for b in both])
        den = functools.reduce(lambda x, y: x + y, [b[1] for b in both])
        accn[tile(t - 1), :] += fold(num)
        accd[tile(t - 1), :] += fold(den)

    open_round(0)

    def inner_filter(t, carry):
        span_rows(t, range(2, nx + 2))
        filtered_rows(t, range(3, nx + 1))
        return carry

    lax.fori_loop(0, nt + 2, inner_filter, 0)

    close_round(0)
    open_round(1)
    half = (nx - 2) // 2

    def inner_stress(i, carry):
        t = i // half + 1
        row = 3 + 2 * lax.rem(i, half)
        stress_row(t, row, True)
        stress_row(t, row + 1, True)
        return carry

    lax.fori_loop(0, nt * half, inner_stress, 0)

    close_round(1)
    open_round(2)

    def inner_sums(t, carry):
        sums(t, range(4, nx))
        return carry

    lax.fori_loop(1, nt + 1, inner_sums, 0)
    close_round(2)

    def later_round(k, carry):
        to_sides(ring.at[k])
        pl.semaphore_wait(ring.at[k], 2)
        return carry

    if rounds > 3:
        lax.fori_loop(3, rounds, later_round, 0)
    to_ends(ring.at[n // 2])
    inner_out = pltpu.make_async_copy(
        strength.at[1:nx - 1], strength_hbm.at[1:nx - 1], out_sem.at[0]
    )
    inner_out.start()

    def rim_first(t):
        span_rows(t, (0, nx + 3), False)
        span_rows(t, (1, nx + 2))
        filtered_rows(t, (1, 2, nx + 1, nx + 2))

    def rim_second(t):
        for row in (1, 2, nx + 1, nx + 2):
            stress_row(t, row, row in (2, nx + 1))
        sums(t, (2, 3, nx, nx + 1))

    def arrive(t, carry):
        x_copy(0, t).wait_recv()
        x_copy(1, t).wait_recv()
        rim_first(t)
        return carry

    lax.fori_loop(1, 1 + EARLY, arrive, 0)
    for side in range(2):
        c_copy(side).wait_recv()
    for side in range(2):
        dst = nx + 2 if side == 0 else 0
        for c in range(3):
            for r in range(2):
                k = 2 * c + r
                u[c, dst + r, 7:8, :] = edge_in[side, k:k + 1, :]
                u[c, dst + r, ny + 8:ny + 9, :] = edge_in[side, 8 + k:9 + k, :]

    def rim_ends(i, carry):
        rim_first(i * (nt + 1))
        return carry

    lax.fori_loop(0, 2, rim_ends, 0)

    def finish(t, carry):
        @pl.when(jnp.logical_and(t > EARLY, t <= nt))
        def _():
            arrive(t, 0)

        rim_second(t - 1)
        return carry

    lax.fori_loop(2, nt + 2, finish, 0)
    rim_out = []
    for k, row in enumerate((0, nx - 1)):
        copy = pltpu.make_async_copy(
            strength.at[row], strength_hbm.at[row], out_sem.at[1 + k]
        )
        copy.start()
        rim_out.append(copy)

    pl.semaphore_wait(ring.at[n // 2], ends)

    mine[0:1, :] = jnp.sum(accn[...].T, axis=0, keepdims=True)
    mine[1:2, :] = jnp.sum(accd[...].T, axis=0, keepdims=True)

    def g_copy(kind, to_x, to_y, from_x):
        return pltpu.make_async_remote_copy(
            src_ref=mine,
            dst_ref=gather.at[kind, from_x],
            send_sem=g_send.at[kind, to_x],
            recv_sem=g_recv.at[kind, from_x],
            device_id=(to_x, to_y),
            device_id_type=MESH,
        )

    def send(i, carry):
        @pl.when(i != gx)
        def _():
            g_copy(0, i, gy, gx).start()

        @pl.when(not_low)
        def _():
            g_copy(2, i, gy - 1, gx).start()

        @pl.when(not_high)
        def _():
            g_copy(1, i, gy + 1, gx).start()

        return carry

    lax.fori_loop(0, n, send, 0)
    gather[0, gx] = mine[...]

    def take(i, carry):
        @pl.when(i != gx)
        def _():
            g_copy(0, i, gy, i).wait_recv()

        @pl.when(not_low)
        def _():
            g_copy(1, i, gy, i).wait_recv()

        @pl.when(not_high)
        def _():
            g_copy(2, i, gy, i).wait_recv()

        return carry

    lax.fori_loop(0, n, take, 0)

    def profile(kind):
        def add(i, total):
            return total + gather[kind, i]

        total = lax.fori_loop(0, n, add, jnp.zeros((2, lanes), jnp.float32))
        return jnp.clip(2.0 * (total[0:1] / total[1:2]), 0.0, clip_high)

    raw = profile(0)
    where = lax.broadcasted_iota(jnp.int32, (1, lanes), 1)
    first = where == 0
    last = where == ny - 1
    under = jnp.where(first, raw, pltpu.roll(raw, 1, 1))
    over = jnp.where(last, raw, pltpu.roll(raw, lanes - 1, 1))
    low_raw = pltpu.roll(profile(1), (lanes + 1 - ny) % lanes, 1)
    high_raw = pltpu.roll(profile(2), ny - 1, 1)
    under = jnp.where(jnp.logical_and(first, not_low), low_raw, under)
    over = jnp.where(jnp.logical_and(last, not_high), high_raw, over)
    coef_ref[...] = 0.25 * under + 0.5 * raw + 0.25 * over

    def left_x(t, carry):
        x_copy(0, t).wait_send()
        x_copy(1, t).wait_send()
        return carry

    lax.fori_loop(1, nt + 1, left_x, 0)
    for side in range(2):
        c_copy(side).wait_send()

    @pl.when(not_low)
    def _():
        y_copy(0).wait_send()

    @pl.when(not_high)
    def _():
        y_copy(1).wait_send()

    def left_g(i, carry):
        @pl.when(i != gx)
        def _():
            g_copy(0, i, gy, gx).wait_send()

        @pl.when(not_low)
        def _():
            g_copy(2, i, gy - 1, gx).wait_send()

        @pl.when(not_high)
        def _():
            g_copy(1, i, gy + 1, gx).wait_send()

        return carry

    lax.fori_loop(0, n, left_g, 0)
    inner_out.wait()
    for copy in rim_out:
        copy.wait()


def local(n, m, velocity):
    _, nx, ny, nz = velocity.shape
    lanes = -(-ny // 128) * 128
    nt = ny // 8
    f32 = jnp.float32
    strength, coef = pl.pallas_call(
        functools.partial(kernel, n, m, nx, ny),
        out_shape=(
            jax.ShapeDtypeStruct((nx, ny, nz), f32),
            jax.ShapeDtypeStruct((1, lanes), f32),
        ),
        in_specs=[pl.BlockSpec(memory_space=pl.ANY)],
        out_specs=(
            pl.BlockSpec(memory_space=pl.ANY),
            pl.BlockSpec(memory_space=pltpu.VMEM),
        ),
        scratch_shapes=[
            pltpu.VMEM((3, nx + 4, ny + 16, nz), f32),
            pltpu.VMEM((3, nx + 4, ny + 16, nz), f32),
            pltpu.VMEM((3, nx + 4, ny + 16, nz), f32),
            pltpu.VMEM((3, nx + 4, ny + 16, nz), f32),
            pltpu.VMEM((6, nx + 4, ny, nz), f32),
            pltpu.VMEM((nx, ny, nz), f32),
            pltpu.VMEM((lanes, 128), f32),
            pltpu.VMEM((lanes, 128), f32),
            pltpu.VMEM((2, 16, nz), f32),
            pltpu.VMEM((2, 16, nz), f32),
            pltpu.VMEM((2, lanes), f32),
            pltpu.VMEM((3, n, 2, lanes), f32),
            pltpu.SemaphoreType.DMA,
            pltpu.SemaphoreType.DMA((3,)),
            pltpu.SemaphoreType.DMA((2, nt)),
            pltpu.SemaphoreType.DMA((2, nt)),
            pltpu.SemaphoreType.DMA((2,)),
            pltpu.SemaphoreType.DMA((2,)),
            pltpu.SemaphoreType.DMA((2,)),
            pltpu.SemaphoreType.DMA((2,)),
            pltpu.SemaphoreType.DMA((3, n)),
            pltpu.SemaphoreType.DMA((3, n)),
            pltpu.SemaphoreType.REGULAR((n // 2 + 1,)),
        ],
        compiler_params=pltpu.CompilerParams(
            collective_id=0, has_side_effects=True, vmem_limit_bytes=67043328
        ),
    )(velocity)
    smooth = coef[0, :ny]
    return (smooth, smooth[None, :, None] * strength)


def solution(mesh):
    n, m = mesh.shape["gx"], mesh.shape["gy"]
    return jax.shard_map(
        functools.partial(local, n, m),
        mesh=mesh,
        in_specs=(P(None, "gx", "gy", None),),
        out_specs=(P("gy"), P("gx", "gy", None)),
        check_vma=False,
    )
```

```python
import functools

import jax
import jax.numpy as jnp
from jax import lax
from jax.experimental import pallas as pl
from jax.experimental.pallas import tpu as pltpu
from jax.sharding import PartitionSpec as P

clip_high = 0.1
pairs = ((0, 0), (1, 1), (2, 2), (0, 1), (0, 2), (1, 2))
MESH = pl.DeviceIdType.MESH
EARLY = 4


def tile(index):
    return pl.ds(pl.multiple_of(index * 8, 8), 8)


def roll_next(value):
    return pltpu.roll(value, value.shape[1] - 1, 1)


def roll_prev(value):
    return pltpu.roll(value, 1, 1)


def filter_span(value):
    return (roll_next(value) + roll_prev(value)) + 2.0 * value


def slope_span(value):
    return roll_next(value) - roll_prev(value)


def slope_wall(ref, comp, row, t, here):
    rows = lax.broadcasted_iota(jnp.int32, here.shape, 0)
    below = ref[comp, row, tile(t - 1), :]
    above = ref[comp, row, tile(t + 1), :]
    up = pltpu.roll(jnp.where(rows == 0, above, here), 7, 0)
    down = pltpu.roll(jnp.where(rows == 7, below, here), 1, 0)
    return up - down


def strain4(ref, row, t, slope=None):
    here = [ref[c, row, tile(t), :] for c in range(3)]
    dx = [ref[c, row + 1, tile(t), :] - ref[c, row - 1, tile(t), :] for c in range(3)]
    dy = [slope_wall(ref, c, row, t, here[c]) for c in range(3)]
    if slope is None:
        dz = [slope_span(here[c]) for c in range(3)]
    else:
        dz = [slope[c, row, tile(t), :] for c in range(3)]
    s = (
        dx[0],
        4.0 * dy[1],
        2.0 * dz[2],
        2.0 * dy[0] + 0.5 * dx[1],
        dz[0] + 0.5 * dx[2],
        dz[1] + 2.0 * dy[2],
    )
    diag = s[0] * s[0] + s[1] * s[1] + s[2] * s[2]
    off = s[3] * s[3] + s[4] * s[4] + s[5] * s[5]
    return here, s, diag + 2.0 * off


def kernel(n, m, nx, ny, u_hbm, strength, coef_ref, u, w, v, d, g, accn, accd,
           edge_out, edge_in, mine, mine_ends, gather, own_sem, xs_send, xs_recv, ys_send, ys_recv,
           c_send, c_recv, g_send, g_recv, ring):
    nt = ny // 8
    gx = lax.axis_index("gx")
    gy = lax.axis_index("gy")
    left, right = lax.rem(gx + n - 1, n), lax.rem(gx + 1, n)
    not_low, not_high = gy > 0, gy < m - 1
    lanes = mine.shape[-1]

    own = pltpu.make_async_copy(u_hbm, u.at[:, 2:2 + nx, 8:8 + ny, :], own_sem)
    own.start()

    barrier = pltpu.get_barrier_semaphore()

    def to_ends(semaphore):
        @pl.when(not_low)
        def _():
            pl.semaphore_signal(semaphore, inc=1, device_id=(gx, gy - 1), device_id_type=MESH)

        @pl.when(not_high)
        def _():
            pl.semaphore_signal(semaphore, inc=1, device_id=(gx, gy + 1), device_id_type=MESH)

    def to_sides(semaphore):
        for side in (left, right):
            pl.semaphore_signal(semaphore, inc=1, device_id=(side, gy), device_id_type=MESH)

    to_sides(barrier)
    to_ends(barrier)
    ends = jnp.where(not_low, 1, 0) + jnp.where(not_high, 1, 0)
    pl.semaphore_wait(barrier, ends + 2)
    own.wait()

    rounds = n // 2 - 1

    def open_round(k):
        if k < rounds:
            to_sides(ring.at[k])

    def close_round(k):
        if k < rounds:
            pl.semaphore_wait(ring.at[k], 2)

    def x_copy(side, t):
        src = 2 if side == 0 else nx
        dst = nx + 2 if side == 0 else 0
        return pltpu.make_async_remote_copy(
            src_ref=u.at[:, src:src + 2, tile(t), :],
            dst_ref=u.at[:, dst:dst + 2, tile(t), :],
            send_sem=xs_send.at[side],
            recv_sem=xs_recv.at[side, t - 1],
            device_id=(left if side == 0 else right, gy),
            device_id_type=MESH,
        )

    def x_all(side):
        part = u.at[:, 2:4, 8:8 + ny, :]
        return pltpu.make_async_remote_copy(
            src_ref=part,
            dst_ref=part,
            send_sem=xs_send.at[side],
            recv_sem=xs_recv.at[side, 0],
            device_id=(right, gy),
            device_id_type=MESH,
        )

    def y_copy(side):
        src = 8 if side == 0 else ny
        dst = ny + 8 if side == 0 else 0
        return pltpu.make_async_remote_copy(
            src_ref=u.at[:, 2:2 + nx, src:src + 8, :],
            dst_ref=u.at[:, 2:2 + nx, dst:dst + 8, :],
            send_sem=ys_send.at[side],
            recv_sem=ys_recv.at[side],
            device_id=(gx, gy - 1 if side == 0 else gy + 1),
            device_id_type=MESH,
        )

    def c_copy(side):
        return pltpu.make_async_remote_copy(
            src_ref=edge_out.at[side],
            dst_ref=edge_in.at[side],
            send_sem=c_send.at[side],
            recv_sem=c_recv.at[side],
            device_id=(left if side == 0 else right, gy),
            device_id_type=MESH,
        )

    @pl.when(not_low)
    def _():
        y_copy(0).start()

    @pl.when(not_high)
    def _():
        y_copy(1).start()

    def start_x(i, carry):
        t = jnp.where(i < 2, nt - i, i - 1)
        x_copy(0, t).start()
        x_copy(1, t).start()
        return carry

    lax.fori_loop(0, EARLY, start_x, 0)

    accn[...] = jnp.zeros_like(accn)
    accd[...] = jnp.zeros_like(accd)

    @pl.when(jnp.logical_not(not_low))
    def _():
        u[:, 2:2 + nx, 0:8, :] = jnp.zeros((3, nx, 8, u.shape[3]), jnp.float32)

    @pl.when(jnp.logical_not(not_high))
    def _():
        u[:, 2:2 + nx, ny + 8:ny + 16, :] = jnp.zeros((3, nx, 8, u.shape[3]), jnp.float32)

    @pl.when(not_high)
    def _():
        y_copy(0).wait_recv()

    @pl.when(not_low)
    def _():
        y_copy(1).wait_recv()

    for side in range(2):
        src = 2 if side == 0 else nx
        for c in range(3):
            for r in range(2):
                k = 2 * c + r
                edge_out[side, k:k + 1, :] = u[c, src + r, 7:8, :]
                edge_out[side, 8 + k:9 + k, :] = u[c, src + r, ny + 8:ny + 9, :]
    for side in range(2):
        c_copy(side).start()
    lax.fori_loop(EARLY, nt, start_x, 0)

    def span_rows(t, rows, slopes=True):
        for c in range(3):
            for row in rows:
                here = u[c, row, tile(t), :]
                after, before = roll_next(here), roll_prev(here)
                w[c, row, tile(t), :] = (after + before) + 2.0 * here
                if slopes:
                    d[c, row, tile(t), :] = after - before

    def filtered_rows(t, rows):
        for c in range(3):
            for row in rows:
                a, b, e = (w[c, row + k, tile(t), :] for k in (-1, 0, 1))
                v[c, row, tile(t), :] = 0.25 * ((a + e) + 2.0 * b)

    def stress_row(t, row, keep):
        _, s, total = strain4(u, row, t, d)
        size = jnp.sqrt(0.125 * total)
        if keep:
            strength[row - 2, tile(t - 1), :] = size
        for k in range(6):
            g[k, row, tile(t - 1), :] = size * s[k]

    def sums_row(t, row):
        centre, s, total = strain4(v, row, t)
        scale = jnp.sqrt(2.0 * total)

        def product(a, b):
            one, two, three = (near[j][a] * near[j][b] for j in range(3))
            return filter_span((one + three) + 2.0 * two)

        def stress(k):
            one, two, three = (g[k, row + j, tile(t - 1), :] for j in (-1, 0, 1))
            return filter_span((one + three) + 2.0 * two)

        near = [[u[c, row + j, tile(t), :] for c in range(3)] for j in (-1, 0, 1)]
        leonard = [product(a, b) - centre[a] * centre[b] for a, b in pairs]
        third = (leonard[0] + leonard[1] + leonard[2]) * (1.0 / 3.0)
        leonard = [x - third for x in leonard[:3]] + leonard[3:]
        model = [stress(k) - scale * s[k] for k in range(6)]
        lm = [x * y for x, y in zip(leonard, model)]
        mm = [x * x for x in model]
        num = (lm[0] + lm[1] + lm[2]) + 2.0 * (lm[3] + lm[4] + lm[5])
        den = (mm[0] + mm[1] + mm[2]) + 2.0 * (mm[3] + mm[4] + mm[5])
        return num, den

    def fold(value):
        parts = [value[:, k:k + 128] for k in range(0, value.shape[1], 128)]
        return functools.reduce(lambda x, y: x + y, parts)

    def sums(t, rows):
        both = [sums_row(t, row) for row in rows]
        num = functools.reduce(lambda x, y: x + y, [b[0] for b in both])
        den = functools.reduce(lambda x, y: x + y, [b[1] for b in both])
        accn[tile(t - 1), :] += fold(num)
        accd[tile(t - 1), :] += fold(den)

    open_round(0)

    def inner_filter(t, carry):
        span_rows(t, range(2, nx + 2))
        filtered_rows(t, range(3, nx + 1))
        return carry

    lax.fori_loop(0, nt + 2, inner_filter, 0)

    close_round(0)
    open_round(1)
    half = (nx - 2) // 2

    def inner_stress(i, carry):
        t = i // half + 1
        row = 3 + 2 * lax.rem(i, half)
        stress_row(t, row, True)
        stress_row(t, row + 1, True)
        return carry

    lax.fori_loop(0, nt * half, inner_stress, 0)

    close_round(1)
    open_round(2)

    def inner_sums(t, carry):
        sums(t, range(4, nx))
        return carry

    lax.fori_loop(1, nt + 1, inner_sums, 0)
    close_round(2)

    def later_round(k, carry):
        to_sides(ring.at[k])
        pl.semaphore_wait(ring.at[k], 2)
        return carry

    if rounds > 3:
        lax.fori_loop(3, rounds, later_round, 0)
    to_ends(ring.at[n // 2])

    def rim_first(t):
        span_rows(t, (0, nx + 3), False)
        span_rows(t, (1, nx + 2))
        filtered_rows(t, (1, 2, nx + 1, nx + 2))

    def rim_second(t):
        for row in (1, 2, nx + 1, nx + 2):
            stress_row(t, row, row in (2, nx + 1))
        sums(t, (2, 3, nx, nx + 1))

    def arrive(t):
        x_copy(0, t).wait_recv()
        x_copy(1, t).wait_recv()
        rim_first(t)

    def arrive_early(i, carry):
        arrive(jnp.where(i < 2, nt - i, i - 1))
        return carry

    lax.fori_loop(0, EARLY, arrive_early, 0)
    for side in range(2):
        c_copy(side).wait_recv()
    for side in range(2):
        dst = nx + 2 if side == 0 else 0
        for c in range(3):
            for r in range(2):
                k = 2 * c + r
                u[c, dst + r, 7:8, :] = edge_in[side, k:k + 1, :]
                u[c, dst + r, ny + 8:ny + 9, :] = edge_in[side, 8 + k:9 + k, :]

    def rim_ends(i, carry):
        rim_first(i * (nt + 1))
        return carry

    lax.fori_loop(0, 2, rim_ends, 0)

    def finish_ends(i, carry):
        rim_second(1 + i * (nt - 1))
        return carry

    lax.fori_loop(0, 2, finish_ends, 0)

    def column_sums(ref):
        ref[0:1, :] = jnp.sum(accn[...].T, axis=0, keepdims=True)
        ref[1:2, :] = jnp.sum(accd[...].T, axis=0, keepdims=True)

    def g_copy(kind, to_x, to_y):
        return pltpu.make_async_remote_copy(
            src_ref=mine if kind == 0 else mine_ends,
            dst_ref=gather.at[kind, gx],
            send_sem=g_send.at[kind],
            recv_sem=g_recv.at[kind],
            device_id=(to_x, to_y),
            device_id_type=MESH,
        )

    def g_all(kind):
        count = n - 1 if kind == 0 else n
        part = gather.at[kind, 0:count]
        return pltpu.make_async_remote_copy(
            src_ref=part,
            dst_ref=part,
            send_sem=g_send.at[kind],
            recv_sem=g_recv.at[kind],
            device_id=(right, gy),
            device_id_type=MESH,
        )

    column_sums(mine_ends)
    pl.semaphore_wait(ring.at[n // 2], ends)

    def send_ends(i, carry):
        @pl.when(not_low)
        def _():
            g_copy(2, i, gy - 1).start()

        @pl.when(not_high)
        def _():
            g_copy(1, i, gy + 1).start()

        return carry

    lax.fori_loop(0, n, send_ends, 0)

    def finish(t, carry):
        @pl.when(t < nt - 1)
        def _():
            arrive(t)

        rim_second(t - 1)
        return carry

    lax.fori_loop(EARLY - 1, nt + 1, finish, 0)

    column_sums(mine)

    def send(i, carry):
        g_copy(0, lax.rem(gx + i, n), gy).start()
        return carry

    lax.fori_loop(1, n, send, 0)
    gather[0, gx] = mine[...]
    g_all(0).wait_recv()

    @pl.when(not_low)
    def _():
        g_all(1).wait_recv()

    @pl.when(not_high)
    def _():
        g_all(2).wait_recv()

    def profile(kind):
        def add(i, total):
            return total + gather[kind, i]

        total = lax.fori_loop(0, n, add, jnp.zeros((2, lanes), jnp.float32))
        return jnp.clip(2.0 * (total[0:1] / total[1:2]), 0.0, clip_high)

    raw = profile(0)
    where = lax.broadcasted_iota(jnp.int32, (1, lanes), 1)
    first = where == 0
    last = where == ny - 1
    under = jnp.where(first, raw, pltpu.roll(raw, 1, 1))
    over = jnp.where(last, raw, pltpu.roll(raw, lanes - 1, 1))
    low_raw = pltpu.roll(profile(1), (lanes + 1 - ny) % lanes, 1)
    high_raw = pltpu.roll(profile(2), ny - 1, 1)
    under = jnp.where(jnp.logical_and(first, not_low), low_raw, under)
    over = jnp.where(jnp.logical_and(last, not_high), high_raw, over)
    coef_ref[...] = 0.25 * under + 0.5 * raw + 0.25 * over

    for side in range(2):
        x_all(side).wait_send()
    for side in range(2):
        c_copy(side).wait_send()

    @pl.when(not_low)
    def _():
        y_copy(0).wait_send()

    @pl.when(not_high)
    def _():
        y_copy(1).wait_send()

    g_all(0).wait_send()

    @pl.when(not_low)
    def _():
        g_all(2).wait_send()

    @pl.when(not_high)
    def _():
        g_all(1).wait_send()


def local(n, m, velocity):
    _, nx, ny, nz = velocity.shape
    lanes = -(-ny // 128) * 128
    nt = ny // 8
    f32 = jnp.float32
    strength, coef = pl.pallas_call(
        functools.partial(kernel, n, m, nx, ny),
        out_shape=(
            jax.ShapeDtypeStruct((nx, ny, nz), f32),
            jax.ShapeDtypeStruct((1, lanes), f32),
        ),
        in_specs=[pl.BlockSpec(memory_space=pltpu.HBM)],
        out_specs=(
            pl.BlockSpec(memory_space=pltpu.VMEM),
            pl.BlockSpec(memory_space=pltpu.VMEM),
        ),
        scratch_shapes=[
            pltpu.VMEM((3, nx + 4, ny + 16, nz), f32),
            pltpu.VMEM((3, nx + 4, ny + 16, nz), f32),
            pltpu.VMEM((3, nx + 4, ny + 16, nz), f32),
            pltpu.VMEM((3, nx + 4, ny + 16, nz), f32),
            pltpu.VMEM((6, nx + 4, ny, nz), f32),
            pltpu.VMEM((lanes, 128), f32),
            pltpu.VMEM((lanes, 128), f32),
            pltpu.VMEM((2, 16, nz), f32),
            pltpu.VMEM((2, 16, nz), f32),
            pltpu.VMEM((2, lanes), f32),
            pltpu.VMEM((2, lanes), f32),
            pltpu.VMEM((3, n, 2, lanes), f32),
            pltpu.SemaphoreType.DMA,
            pltpu.SemaphoreType.DMA((2,)),
            pltpu.SemaphoreType.DMA((2, nt)),
            pltpu.SemaphoreType.DMA((2,)),
            pltpu.SemaphoreType.DMA((2,)),
            pltpu.SemaphoreType.DMA((2,)),
            pltpu.SemaphoreType.DMA((2,)),
            pltpu.SemaphoreType.DMA((3,)),
            pltpu.SemaphoreType.DMA((3,)),
            pltpu.SemaphoreType.REGULAR((n // 2 + 1,)),
        ],
        compiler_params=pltpu.CompilerParams(
            collective_id=0, has_side_effects=True, vmem_limit_bytes=32 * 1024 * 1024
        ),
    )(pltpu.with_memory_space_constraint(velocity, pltpu.HBM))
    smooth = coef[0, :ny]
    return (smooth, smooth[None, :, None] * strength)


def solution(mesh):
    n, m = mesh.shape["gx"], mesh.shape["gy"]
    return jax.shard_map(
        functools.partial(local, n, m),
        mesh=mesh,
        in_specs=(P(None, "gx", "gy", None),),
        out_specs=(P("gy"), P("gx", "gy", None)),
        check_vma=False,
    )
```
